32 devices in a mesh: section: 4 (over z), seq: 8 (over y, x, core).
Axes of the slice: x: 2, y: 2, z: 4, core: 2. Of those that a mesh axis runs over, the one named last changes fastest.
Arguments:
- saved: bfloat16 [4, 3, 1024, 2304], P('section', None, 'seq'), may hold values from -8 to 8
- cotangent: bfloat16 [3, 1024, 2304], P(None, 'seq'), may hold values from -0.109375 to 0.109375
- slot_table: int32 [4, 3], P('section'), may hold values from 0 to 2, each once within a row
- gain: float32 [4, 2304], P('section'), may hold values from 0.25 to 1.75
- value_weight: bfloat16 [4, 2304, 1024], P('section'), may hold values from -0.125 to 0.125
- out_weight: bfloat16 [4, 2304, 1024], P('section'), may hold values from -0.1875 to 0.1875
Outputs:
- value_grad: float32 [4, 2304, 1024], P('section', 'seq')
- out_grad: float32 [4, 2304, 1024], P('section', 'seq')
- gain_grad: float32 [4, 2304], P('section')
The draws below stay inside these ranges and needn't reach their ends.
Inputs may be any that keep to these rules, and one draw needn't show every extreme that they name: `slot_table`: each row names every stash slot once.
All inputs are finite; a program needn't handle non-finite values.
Results may differ from the reference program's by a relative error of at most 0.007.
Values may be sent and summed in bfloat16 or wider, within the bound.
A program may use at most 128 MiB of HBM per device.

```python
import jax
import jax.numpy as jnp
from jax import lax

D = 2304
R = 1024
MICRO = 3
TOKENS = 1024
N_SECTION = 4


def strengthened(entries, own_key, source, target, shards_of, factor):
    owner, partner = [(jnp.arange(entries.shape[dim]) // (entries.shape[dim] // shards_of)).reshape([-1 if axis == dim else 1 for axis in range(entries.ndim)]) for dim in (source, target)]
    chosen = jax.random.permutation(own_key, shards_of)[partner]
    strong = (owner == chosen) | (owner == (partner + shards_of // 2) % shards_of)
    return jnp.where(strong, factor * entries, entries)


def block_scale(own_key, dims, pieces, low, high):
    loudness = 1.0
    for axis_at, shards_of in pieces:
        steps = jax.random.uniform(jax.random.fold_in(jax.random.fold_in(own_key, 6), axis_at), (shards_of,), jnp.float32, low / len(pieces), high / len(pieces))
        loudness = loudness * jnp.repeat(jnp.exp(steps), dims[axis_at] // shards_of).reshape((-1,) + (1,) * (len(dims) - 1 - axis_at))
    return loudness


def bell_draw(key, extent, spread, limit, shards=(), held_as=jnp.bfloat16):
    entries = spread * jax.random.normal(key, extent, jnp.float32)
    if shards:
        entries = entries * block_scale(key, extent, shards, -0.22, 0.18)
    return jnp.clip(entries, -limit, limit).astype(held_as)


def bell_draw_with(rng, extent, scale, most, shards, heavy, kind=jnp.bfloat16):
    drawn = scale * jax.random.normal(rng, extent, jnp.float32)
    if shards:
        drawn = drawn * block_scale(rng, extent, shards, -0.22, 0.18)
    return jnp.clip(strengthened(drawn, jax.random.fold_in(rng, 3), *heavy), -most, most).astype(kind)


def setup_inputs(seed: int = 0) -> dict:
    splits = jax.random.split(jax.random.key(seed), 7)
    return {
        "saved": bell_draw_with(splits[0], (N_SECTION, MICRO, TOKENS, D), 1.0, 8.0, ((0, 4), (2, 8)), (2, 3, 8, 2.0)),
        "cotangent": bell_draw(splits[1], (MICRO, TOKENS, D), ((MICRO * TOKENS) ** -0.5), 0.109375, ((1, 8),)),
        "slot_table": jax.vmap(lambda own: jax.random.permutation(own, MICRO))(jax.random.split(splits[2], N_SECTION)).reshape((N_SECTION, MICRO)).astype(jnp.int32),
        "gain": jnp.clip(1.0 + 0.15 * jax.random.normal(splits[3], (N_SECTION, D), jnp.float32), 0.25, 1.75),
        "value_weight": bell_draw(splits[4], (N_SECTION, D, R), D ** -0.5, 0.125, ((0, 4),)),
        "out_weight": bell_draw(splits[5], (N_SECTION, D, R), R ** -0.5, 0.1875, ((0, 4),)),
    }


EPSILON = 1e-06

def normalize(inputs, gain_row):
    value_rows = inputs.astype(jnp.float32)
    inv_rms = lax.rsqrt(lax.optimization_barrier(jnp.mean(value_rows * value_rows, axis=-1, keepdims=True)) + EPSILON)
    unit_rows = value_rows * inv_rms
    return (unit_rows, inv_rms, (unit_rows * gain_row).astype(jnp.bfloat16))

def layer_backward(inputs, grad_out, gain_row, w_value, w_out):
    unit_rows, inv_rms, normed = normalize(inputs, gain_row)
    value_out = jnp.dot(normed, w_value, preferred_element_type=jnp.float32).astype(jnp.bfloat16)
    grad_value = jnp.dot(grad_out, w_out, preferred_element_type=jnp.float32).astype(jnp.bfloat16)
    grad_normed = lax.dot_general(grad_value, w_value, (((1,), (1,)), ((), ())), preferred_element_type=jnp.float32)
    gain_term = lax.optimization_barrier(jnp.sum(grad_normed * unit_rows, axis=0))
    grad_unit = grad_normed * gain_row
    grad_in = grad_out.astype(jnp.float32) + inv_rms * (grad_unit - unit_rows * lax.optimization_barrier(jnp.mean(grad_unit * unit_rows, axis=-1, keepdims=True)))
    value_term = lax.dot_general(normed, grad_value, (((0,), (0,)), ((), ())), preferred_element_type=jnp.float32)
    out_term = lax.dot_general(grad_out, value_out, (((0,), (0,)), ((), ())), preferred_element_type=jnp.float32)
    return (grad_in.astype(jnp.bfloat16), gain_term, value_term, out_term)

def reference(saved, cotangent, slot_table, gain, value_weight, out_weight):
    grads = [cotangent[micro_index] for micro_index in range(MICRO)]
    value_list = []
    out_list = []
    gain_list = []
    for section_index in reversed(range(N_SECTION)):
        value_acc = jnp.zeros((D, R), jnp.float32)
        out_acc = jnp.zeros((D, R), jnp.float32)
        gain_acc = jnp.zeros((D,), jnp.float32)
        next_grads = []
        for micro_index in range(MICRO):
            slot_index = slot_table[section_index, micro_index].astype(jnp.int32)
            inputs = lax.dynamic_index_in_dim(saved[section_index], slot_index, 0, keepdims=False)
            grad_in, gain_term, value_term, out_term = layer_backward(inputs, grads[micro_index], gain[section_index], value_weight[section_index], out_weight[section_index])
            value_acc = value_acc + value_term
            out_acc = out_acc + out_term
            gain_acc = gain_acc + gain_term
            next_grads.append(grad_in)
        grads = next_grads
        value_list.insert(0, value_acc)
        out_list.insert(0, out_acc)
        gain_list.insert(0, gain_acc)
    return (jnp.stack(value_list), jnp.stack(out_list), jnp.stack(gain_list))
```

```python
import functools

import jax
import jax.numpy as jnp
from jax import lax
from jax.experimental import pallas as pl
from jax.experimental.pallas import tpu as pltpu
from jax.sharding import PartitionSpec as P

EPSILON = 1e-06


def passed_along(value, axis, steps):
    count = lax.axis_size(axis)
    first, last = (max(0, -steps), min(count, count - steps))
    return lax.ppermute(value, axis, [(source, source + steps) for source in range(first, last)])


def normalize(inputs, gain_row):
    value_rows = inputs.astype(jnp.float32)
    inv_rms = lax.rsqrt(jnp.mean(value_rows * value_rows, axis=-1, keepdims=True) + EPSILON)
    unit_rows = value_rows * inv_rms
    return (unit_rows, inv_rms, (unit_rows * gain_row).astype(jnp.bfloat16))


def input_grads(inputs, grad_out, gain_row, w_value, w_out):
    unit_rows, inv_rms, normed = normalize(inputs, gain_row)
    grad_value = jnp.dot(grad_out, w_out, preferred_element_type=jnp.float32).astype(jnp.bfloat16)
    grad_normed = lax.dot_general(
        grad_value, w_value, (((1,), (1,)), ((), ())), preferred_element_type=jnp.float32
    )
    gain_term = jnp.sum(grad_normed * unit_rows, axis=0)
    grad_unit = grad_normed * gain_row
    grad_in = grad_out.astype(jnp.float32) + inv_rms * (
        grad_unit - unit_rows * jnp.mean(grad_unit * unit_rows, axis=-1, keepdims=True)
    )
    return (grad_in.astype(jnp.bfloat16), grad_value, normed, gain_term)


def arrivals(
    step_index, sent, section_count, section_index, micro_count, cotangent, local_saved, slot_order
):
    if step_index > 0:
        incoming = passed_along(sent, "section", -1)
    else:
        incoming = sent
    micro_index = step_index - (section_count - 1 - section_index)
    active_now = jnp.logical_and(micro_index >= 0, micro_index < micro_count)
    clipped = jnp.clip(micro_index, 0, micro_count - 1)
    top_grad = lax.dynamic_index_in_dim(cotangent, clipped, 0, keepdims=False)
    grad_out = jnp.where(section_index == section_count - 1, top_grad, incoming)
    slot_index = lax.dynamic_index_in_dim(slot_order, clipped, 0, keepdims=False)
    inputs = lax.dynamic_index_in_dim(local_saved, slot_index, 0, keepdims=False)
    return (active_now, clipped, grad_out, inputs)


def per_device(saved, cotangent, slot_table, gain, value_weight, out_weight):
    section_count = lax.axis_size("section")
    section_index = lax.axis_index("section")
    micro_count = slot_table.shape[1]
    local_saved = saved[0]
    slot_order = slot_table[0]
    gain_row = gain[0]
    w_value = value_weight[0]
    w_out = out_weight[0]
    token_rows = cotangent.shape[1]
    model_width = w_value.shape[0]
    inner_width = w_value.shape[1]
    sent = jnp.zeros((token_rows, model_width), jnp.bfloat16)
    gain_acc = jnp.zeros((model_width,), jnp.float32)
    out_stash = jnp.zeros((micro_count, token_rows, model_width), jnp.bfloat16)
    value_stash = jnp.zeros((micro_count, token_rows, inner_width), jnp.bfloat16)
    for step_index in range(micro_count + section_count - 1):
        active_now, clipped, grad_out, inputs = arrivals(
            step_index,
            sent,
            section_count,
            section_index,
            micro_count,
            cotangent,
            local_saved,
            slot_order,
        )

        def working(carried):
            grad_in, grad_value, normed, gain_term = input_grads(
                inputs, grad_out, gain_row, w_value, w_out
            )
            new_out = lax.dynamic_update_index_in_dim(carried[2], grad_out, clipped, 0)
            new_value = lax.dynamic_update_index_in_dim(carried[3], grad_value, clipped, 0)
            return (grad_in, carried[1] + gain_term, new_out, new_value)

        def resting(carried):
            return carried

        sent, gain_acc, out_stash, value_stash = lax.cond(
            active_now, working, resting, (sent, gain_acc, out_stash, value_stash)
        )
    ordered = jnp.take(local_saved, slot_order, axis=0).reshape(
        micro_count * token_rows, model_width
    )
    unit_all, inv_all, normed_all = normalize(ordered, gain_row)
    values_all = jnp.dot(normed_all, w_value, preferred_element_type=jnp.float32).astype(
        jnp.bfloat16
    )
    grads_all = out_stash.reshape(micro_count * token_rows, model_width)
    grad_values = value_stash.reshape(micro_count * token_rows, inner_width)
    value_acc = lax.dot_general(
        normed_all, grad_values, (((0,), (0,)), ((), ())), preferred_element_type=jnp.float32
    )
    out_acc = lax.dot_general(
        grads_all, values_all, (((0,), (0,)), ((), ())), preferred_element_type=jnp.float32
    )
    value_grad, out_grad = (
        lax.psum_scatter(value_acc, "seq", scatter_dimension=0, tiled=True),
        lax.psum_scatter(out_acc, "seq", scatter_dimension=0, tiled=True),
    )
    gain_total = lax.psum(gain_acc, "seq")
    return (value_grad[None], out_grad[None], gain_total[None])


TILE = 256
LANES = 128
VMEM_BYTES = 60 * 1024 * 1024


def flipped(index, bits, count):
    total, unit = 0, 1
    while unit < count:
        total = total + ((index // unit + (bits // unit) % 2) % 2) * unit
        unit *= 2
    return total


def tile_at(index, size=TILE):
    return pl.ds(pl.multiple_of(index * size, size), size)


def fused_kernel(
    peers,
    sections,
    slot_ref,
    saved_ref,
    cot_ref,
    gain_ref,
    wv_ref,
    wo_ref,
    vg_ref,
    og_ref,
    gg_ref,
    inv_buf,
    grad_buf,
    pass_buf,
    gn_buf,
    rows_all,
    turned,
    cols_all,
    gain_all,
    rows_send,
    rows_recv,
    cols_send,
    cols_recv,
    down_send,
    down_recv,
    gain_send,
    gain_recv,
):
    section = lax.axis_index("section")
    me = lax.axis_index("seq")
    micro, tokens, width = cot_ref.shape
    inner = wv_ref.shape[1]
    share = width // peers
    wide, narrow = width // TILE, inner // TILE
    top = section == sections - 1

    def peer(bits):
        return {"seq": flipped(me, bits, peers)}

    def row_copy(kind, m, owner, sem, target):
        place = rows_all.at[kind, m, tile_at(owner, tokens)]
        return pltpu.make_async_remote_copy(
            src_ref=place,
            dst_ref=place,
            send_sem=rows_send.at[kind, m, sem],
            recv_sem=rows_recv.at[kind, m, sem],
            device_id=target,
            device_id_type=pl.DeviceIdType.MESH,
        )

    def own_rows(kind, m, bits):
        return row_copy(kind, m, me, bits, peer(bits))

    def relayed_rows(kind, m, bits):
        return row_copy(kind, m, flipped(me, bits, peers), bits + 1, peer(1))

    def arriving_rows(kind, m, bits):
        return row_copy(kind, m, flipped(me, bits, peers), bits, peer(bits))

    def col_copy(kind, m, owner, bits):
        return pltpu.make_async_remote_copy(
            src_ref=turned.at[kind, m, tile_at(flipped(me, bits, peers), share)],
            dst_ref=cols_all.at[kind, m, :, tile_at(owner, tokens)],
            send_sem=cols_send.at[kind, m, bits],
            recv_sem=cols_recv.at[kind, m, bits],
            device_id=peer(bits),
            device_id_type=pl.DeviceIdType.MESH,
        )

    def down_copy(m, target):
        return pltpu.make_async_remote_copy(
            src_ref=pass_buf.at[m],
            dst_ref=grad_buf.at[m],
            send_sem=down_send.at[m],
            recv_sem=down_recv.at[m],
            device_id={"section": target},
            device_id_type=pl.DeviceIdType.MESH,
        )

    def gain_copy(owner, bits):
        return pltpu.make_async_remote_copy(
            src_ref=gain_all.at[owner],
            dst_ref=gain_all.at[owner],
            send_sem=gain_send.at[bits],
            recv_sem=gain_recv.at[bits],
            device_id=peer(bits),
            device_id_type=pl.DeviceIdType.MESH,
        )

    barrier = pltpu.get_barrier_semaphore()
    for bits in range(1, peers):
        pl.semaphore_signal(
            barrier, inc=1, device_id=peer(bits), device_id_type=pl.DeviceIdType.MESH
        )

    @pl.when(section > 0)
    def _():
        pl.semaphore_signal(
            barrier,
            inc=1,
            device_id={"section": section - 1},
            device_id_type=pl.DeviceIdType.MESH,
        )

    @pl.when(section < sections - 1)
    def _():
        pl.semaphore_signal(
            barrier,
            inc=1,
            device_id={"section": section + 1},
            device_id_type=pl.DeviceIdType.MESH,
        )

    pl.semaphore_wait(
        barrier,
        peers - 1
        + (section > 0).astype(jnp.int32)
        + (section < sections - 1).astype(jnp.int32),
    )

    gain_all[me] = jnp.zeros((1, width), jnp.float32)
    vg_ref[...] = jnp.zeros_like(vg_ref)
    og_ref[...] = jnp.zeros_like(og_ref)

    def scales(m, carry):
        slot = slot_ref[0, m]

        def squares(j, total):
            x = saved_ref[slot, :, tile_at(j)].astype(jnp.float32)
            return total + jnp.sum(x * x, axis=1, keepdims=True)

        total = lax.fori_loop(0, wide, squares, jnp.zeros((tokens, 1), jnp.float32))
        inv_buf[m] = lax.rsqrt(total / width + EPSILON)
        return carry

    lax.fori_loop(0, micro, scales, 0)

    def send_cols(kind, m):
        cols_all[kind, m, :, tile_at(me, tokens)] = turned[kind, m, tile_at(me, share)]
        for bits in range(1, peers):
            col_copy(kind, m, me, bits).start()

    def send_rows(kind, m):
        for bits in (*range(2, peers, 2), 1):
            own_rows(kind, m, bits).start()

    def values(m):
        slot = slot_ref[0, m]
        inv = inv_buf[m]

        def norm(j, carry):
            x = saved_ref[slot, :, tile_at(j)].astype(jnp.float32)
            n = (x * inv * gain_ref[:, tile_at(j)]).astype(jnp.bfloat16)
            pass_tile[:, tile_at(j)] = n
            turned[0, m, tile_at(j)] = n.T
            return carry

        lax.fori_loop(0, wide, norm, 0)
        send_cols(0, m)

        def project(j, carry):
            rows_all[0, m, tile_at(me, tokens), tile_at(j)] = jnp.dot(
                pass_tile[...], wv_ref[:, tile_at(j)], preferred_element_type=jnp.float32
            ).astype(jnp.bfloat16)
            return carry

        lax.fori_loop(0, narrow, project, 0)
        send_rows(0, m)

    pass_tile = gn_buf[0]
    gn = gn_buf[1]

    def chain(m):
        slot = slot_ref[0, m]
        inv = inv_buf[m]

        @pl.when(top)
        def _():
            grad_buf[m] = cot_ref[m]

        @pl.when(section < sections - 1)
        def _():
            down_copy(m, section + 1).wait_recv()

        def project(j, carry):
            rows_all[1, m, tile_at(me, tokens), tile_at(j)] = jnp.dot(
                grad_buf[m], wo_ref[:, tile_at(j)], preferred_element_type=jnp.float32
            ).astype(jnp.bfloat16)
            return carry

        lax.fori_loop(0, narrow, project, 0)
        send_rows(1, m)

        def back(j, total):
            term = lax.dot_general(
                rows_all[1, m, tile_at(me, tokens)],
                wv_ref[tile_at(j)],
                (((1,), (1,)), ((), ())),
                preferred_element_type=jnp.float32,
            )
            unit = saved_ref[slot, :, tile_at(j)].astype(jnp.float32) * inv
            gn[:, tile_at(j)] = term
            both = term * unit
            gain_all[me, :, tile_at(j)] += jnp.sum(both, axis=0, keepdims=True)
            return total + jnp.sum(both * gain_ref[:, tile_at(j)], axis=1, keepdims=True)

        total = lax.fori_loop(0, wide, back, jnp.zeros((tokens, 1), jnp.float32))
        mean = total / width

        @pl.when(section > 0)
        def _():
            def step(j, carry):
                unit = saved_ref[slot, :, tile_at(j)].astype(jnp.float32) * inv
                grad_unit = gn[:, tile_at(j)] * gain_ref[:, tile_at(j)]
                pass_buf[m, :, tile_at(j)] = (
                    grad_buf[m, :, tile_at(j)].astype(jnp.float32)
                    + inv * (grad_unit - unit * mean)
                ).astype(jnp.bfloat16)
                return carry

            lax.fori_loop(0, wide, step, 0)
            down_copy(m, section - 1).start()

        def turn(j, carry):
            turned[1, m, tile_at(j)] = grad_buf[m, :, tile_at(j)].T
            return carry

        lax.fori_loop(0, wide, turn, 0)
        send_cols(1, m)

    def stage(t, carry):
        at_top = top.astype(jnp.int32)
        chained = at_top * (1 - t % 2) + (1 - at_top) * (t // micro)
        m = at_top * (t // 2) + (1 - at_top) * (t % micro)

        @pl.when(chained == 1)
        def _():
            chain(m)

        @pl.when(chained == 0)
        def _():
            values(m)

        return carry

    lax.fori_loop(0, 2 * micro, stage, 0)
    for bits in range(1, peers):
        gain_copy(me, bits).start()

    def finish(m, carry):
        for kind in (0, 1):
            for bits in range(2, peers, 2):
                arriving_rows(kind, m, bits).wait_recv()
                relayed_rows(kind, m, bits).start()
        for kind in (0, 1):
            for bits in range(1, peers):
                col_copy(kind, m, flipped(me, bits, peers), bits).wait_recv()
        for kind in (0, 1):
            for bits in range(1, peers, 2):
                arriving_rows(kind, m, bits).wait_recv()

        def weight(j, inside):
            vg_ref[:, tile_at(j)] += jnp.dot(
                cols_all[0, m], rows_all[1, m, :, tile_at(j)], preferred_element_type=jnp.float32
            )
            og_ref[:, tile_at(j)] += jnp.dot(
                cols_all[1, m], rows_all[0, m, :, tile_at(j)], preferred_element_type=jnp.float32
            )
            return inside

        lax.fori_loop(0, narrow, weight, 0)
        return carry

    lax.fori_loop(0, micro, finish, 0)
    for bits in range(1, peers):
        gain_copy(flipped(me, bits, peers), bits).wait_recv()
    gained = gain_all[0]
    for owner in range(1, peers):
        gained = gained + gain_all[owner]
    gg_ref[...] = gained

    def drain(m, carry):
        for kind in (0, 1):
            for bits in range(1, peers):
                col_copy(kind, m, me, bits).wait_send()
            for bits in (1, *range(2, peers, 2)):
                own_rows(kind, m, bits).wait_send()
            for bits in range(2, peers, 2):
                relayed_rows(kind, m, bits).wait_send()

        @pl.when(section > 0)
        def _():
            down_copy(m, section - 1).wait_send()

        return carry

    lax.fori_loop(0, micro, drain, 0)
    for bits in range(1, peers):
        gain_copy(me, bits).wait_send()


def fused(mesh, saved, cotangent, slot_table, gain, value_weight, out_weight):
    peers, sections = mesh.shape["seq"], mesh.shape["section"]
    micro, tokens, width = cotangent.shape
    inner = value_weight.shape[2]
    share = width // peers
    hbm = pl.BlockSpec(memory_space=pltpu.VMEM)
    value_grad, out_grad, gain_grad = pl.pallas_call(
        functools.partial(fused_kernel, peers, sections),
        out_shape=(
            jax.ShapeDtypeStruct((share, inner), jnp.float32),
            jax.ShapeDtypeStruct((share, inner), jnp.float32),
            jax.ShapeDtypeStruct((1, width), jnp.float32),
        ),
        in_specs=[pl.BlockSpec(memory_space=pltpu.SMEM)] + [hbm] * 5,
        out_specs=(hbm, hbm, hbm),
        scratch_shapes=[
            pltpu.VMEM((micro, tokens, 1), jnp.float32),
            pltpu.VMEM((micro, tokens, width), jnp.bfloat16),
            pltpu.VMEM((micro, tokens, width), jnp.bfloat16),
            (pltpu.VMEM((tokens, width), jnp.bfloat16), pltpu.VMEM((tokens, width), jnp.float32)),
            pltpu.VMEM((2, micro, peers * tokens, inner), jnp.bfloat16),
            pltpu.VMEM((2, micro, width, tokens), jnp.bfloat16),
            pltpu.VMEM((2, micro, share, peers * tokens), jnp.bfloat16),
            pltpu.VMEM((peers, 1, width), jnp.float32),
            pltpu.SemaphoreType.DMA((2, micro, peers)),
            pltpu.SemaphoreType.DMA((2, micro, peers)),
            pltpu.SemaphoreType.DMA((2, micro, peers)),
            pltpu.SemaphoreType.DMA((2, micro, peers)),
            pltpu.SemaphoreType.DMA((micro,)),
            pltpu.SemaphoreType.DMA((micro,)),
            pltpu.SemaphoreType.DMA((peers,)),
            pltpu.SemaphoreType.DMA((peers,)),
        ],
        compiler_params=pltpu.CompilerParams(
            collective_id=0, has_side_effects=True, vmem_limit_bytes=VMEM_BYTES
        ),
    )(slot_table, saved[0], cotangent, gain, value_weight[0], out_weight[0])
    return value_grad[None], out_grad[None], gain_grad


def fits(mesh, saved, cotangent, slot_table, gain, value_weight, out_weight):
    peers = mesh.shape["seq"]
    micro, tokens, width = cotangent.shape
    inner = value_weight.shape[2]
    held = 4 * width * inner + 4 * micro * tokens * (2 * width + inner * peers)
    held += 4 * micro * tokens * width * 3 + 8 * (width // peers) * inner + 6 * tokens * width
    return (
        peers & (peers - 1) == 0
        and tokens % LANES == 0
        and width % TILE == 0
        and inner % TILE == 0
        and width % (16 * peers) == 0
        and held < VMEM_BYTES - 4 * 1024 * 1024
    )


def on_device(mesh, *arrays):
    if fits(mesh, *arrays):
        return fused(mesh, *arrays)
    return per_device(*arrays)


def solution(mesh):
    in_specs = (
        P("section", None, "seq", None),
        P(None, "seq", None),
        P("section", None),
        P("section", None),
        P("section", None, None),
        P("section", None, None),
    )
    out_specs = (P("section", "seq", None), P("section", "seq", None), P("section", None))
    return jax.shard_map(
        functools.partial(on_device, mesh), mesh=mesh, in_specs=in_specs, out_specs=out_specs, check_vma=False
    )
```

```python
import functools

import jax
import jax.numpy as jnp
from jax import lax
from jax.experimental import pallas as pl
from jax.experimental.pallas import tpu as pltpu
from jax.sharding import PartitionSpec as P

EPSILON = 1e-06


def passed_along(value, axis, steps):
    count = lax.axis_size(axis)
    first, last = (max(0, -steps), min(count, count - steps))
    return lax.ppermute(value, axis, [(source, source + steps) for source in range(first, last)])


def normalize(inputs, gain_row):
    value_rows = inputs.astype(jnp.float32)
    inv_rms = lax.rsqrt(jnp.mean(value_rows * value_rows, axis=-1, keepdims=True) + EPSILON)
    unit_rows = value_rows * inv_rms
    return (unit_rows, inv_rms, (unit_rows * gain_row).astype(jnp.bfloat16))


def input_grads(inputs, grad_out, gain_row, w_value, w_out):
    unit_rows, inv_rms, normed = normalize(inputs, gain_row)
    grad_value = jnp.dot(grad_out, w_out, preferred_element_type=jnp.float32).astype(jnp.bfloat16)
    grad_normed = lax.dot_general(
        grad_value, w_value, (((1,), (1,)), ((), ())), preferred_element_type=jnp.float32
    )
    gain_term = jnp.sum(grad_normed * unit_rows, axis=0)
    grad_unit = grad_normed * gain_row
    grad_in = grad_out.astype(jnp.float32) + inv_rms * (
        grad_unit - unit_rows * jnp.mean(grad_unit * unit_rows, axis=-1, keepdims=True)
    )
    return (grad_in.astype(jnp.bfloat16), grad_value, normed, gain_term)


def arrivals(
    step_index, sent, section_count, section_index, micro_count, cotangent, local_saved, slot_order
):
    if step_index > 0:
        incoming = passed_along(sent, "section", -1)
    else:
        incoming = sent
    micro_index = step_index - (section_count - 1 - section_index)
    active_now = jnp.logical_and(micro_index >= 0, micro_index < micro_count)
    clipped = jnp.clip(micro_index, 0, micro_count - 1)
    top_grad = lax.dynamic_index_in_dim(cotangent, clipped, 0, keepdims=False)
    grad_out = jnp.where(section_index == section_count - 1, top_grad, incoming)
    slot_index = lax.dynamic_index_in_dim(slot_order, clipped, 0, keepdims=False)
    inputs = lax.dynamic_index_in_dim(local_saved, slot_index, 0, keepdims=False)
    return (active_now, clipped, grad_out, inputs)


def per_device(saved, cotangent, slot_table, gain, value_weight, out_weight):
    section_count = lax.axis_size("section")
    section_index = lax.axis_index("section")
    micro_count = slot_table.shape[1]
    local_saved = saved[0]
    slot_order = slot_table[0]
    gain_row = gain[0]
    w_value = value_weight[0]
    w_out = out_weight[0]
    token_rows = cotangent.shape[1]
    model_width = w_value.shape[0]
    inner_width = w_value.shape[1]
    sent = jnp.zeros((token_rows, model_width), jnp.bfloat16)
    gain_acc = jnp.zeros((model_width,), jnp.float32)
    out_stash = jnp.zeros((micro_count, token_rows, model_width), jnp.bfloat16)
    value_stash = jnp.zeros((micro_count, token_rows, inner_width), jnp.bfloat16)
    for step_index in range(micro_count + section_count - 1):
        active_now, clipped, grad_out, inputs = arrivals(
            step_index,
            sent,
            section_count,
            section_index,
            micro_count,
            cotangent,
            local_saved,
            slot_order,
        )

        def working(carried):
            grad_in, grad_value, normed, gain_term = input_grads(
                inputs, grad_out, gain_row, w_value, w_out
            )
            new_out = lax.dynamic_update_index_in_dim(carried[2], grad_out, clipped, 0)
            new_value = lax.dynamic_update_index_in_dim(carried[3], grad_value, clipped, 0)
            return (grad_in, carried[1] + gain_term, new_out, new_value)

        def resting(carried):
            return carried

        sent, gain_acc, out_stash, value_stash = lax.cond(
            active_now, working, resting, (sent, gain_acc, out_stash, value_stash)
        )
    ordered = jnp.take(local_saved, slot_order, axis=0).reshape(
        micro_count * token_rows, model_width
    )
    unit_all, inv_all, normed_all = normalize(ordered, gain_row)
    values_all = jnp.dot(normed_all, w_value, preferred_element_type=jnp.float32).astype(
        jnp.bfloat16
    )
    grads_all = out_stash.reshape(micro_count * token_rows, model_width)
    grad_values = value_stash.reshape(micro_count * token_rows, inner_width)
    value_acc = lax.dot_general(
        normed_all, grad_values, (((0,), (0,)), ((), ())), preferred_element_type=jnp.float32
    )
    out_acc = lax.dot_general(
        grads_all, values_all, (((0,), (0,)), ((), ())), preferred_element_type=jnp.float32
    )
    value_grad, out_grad = (
        lax.psum_scatter(value_acc, "seq", scatter_dimension=0, tiled=True),
        lax.psum_scatter(out_acc, "seq", scatter_dimension=0, tiled=True),
    )
    gain_total = lax.psum(gain_acc, "seq")
    return (value_grad[None], out_grad[None], gain_total[None])


TILE = 256
PIECES = 2
LANES = 128
VMEM_BYTES = 60 * 1024 * 1024


def flipped(index, bits, count):
    total, unit = 0, 1
    while unit < count:
        total = total + ((index // unit + (bits // unit) % 2) % 2) * unit
        unit *= 2
    return total


def tile_at(index, size=TILE):
    return pl.ds(pl.multiple_of(index * size, size), size)


def fused_kernel(
    peers,
    sections,
    slot_ref,
    saved_ref,
    cot_ref,
    gain_ref,
    wv_hbm,
    wo_hbm,
    vg_ref,
    og_ref,
    gg_ref,
    inv_buf,
    grad_buf,
    pass_buf,
    gn_buf,
    rows_all,
    turned,
    cols_all,
    gain_all,
    rows_send,
    rows_recv,
    cols_send,
    cols_recv,
    down_send,
    down_recv,
    gain_send,
    gain_recv,
    wv_ref,
    wo_ref,
    load_sem,
):
    loads = (
        pltpu.make_async_copy(wo_hbm, wo_ref, load_sem.at[0]),
        pltpu.make_async_copy(wv_hbm, wv_ref, load_sem.at[1]),
    )
    for load in loads:
        load.start()
    section = lax.axis_index("section")
    me = lax.axis_index("seq")
    micro, tokens, width = cot_ref.shape
    inner = wv_ref.shape[1]
    share = width // peers
    wide, narrow = width // TILE, inner // TILE
    top = section == sections - 1

    def peer(bits):
        return {"seq": flipped(me, bits, peers)}

    def row_copy(kind, m, owner, sem, target):
        place = rows_all.at[kind, m, tile_at(owner, tokens)]
        return pltpu.make_async_remote_copy(
            src_ref=place,
            dst_ref=place,
            send_sem=rows_send.at[kind, m, sem],
            recv_sem=rows_recv.at[kind, m, sem],
            device_id=target,
            device_id_type=pl.DeviceIdType.MESH,
        )

    def own_rows(kind, m, bits):
        return row_copy(kind, m, me, bits, peer(bits))

    def relayed_rows(kind, m, bits):
        return row_copy(kind, m, flipped(me, bits, peers), bits + 1, peer(1))

    def arriving_rows(kind, m, bits):
        return row_copy(kind, m, flipped(me, bits, peers), bits, peer(bits))

    def col_copy(kind, m, owner, bits):
        return pltpu.make_async_remote_copy(
            src_ref=turned.at[kind, m, tile_at(flipped(me, bits, peers), share)],
            dst_ref=cols_all.at[kind, m, :, tile_at(owner, tokens)],
            send_sem=cols_send.at[kind, m, bits],
            recv_sem=cols_recv.at[kind, m, bits],
            device_id=peer(bits),
            device_id_type=pl.DeviceIdType.MESH,
        )

    piece = tokens // PIECES

    def down_copy(m, h, target):
        return pltpu.make_async_remote_copy(
            src_ref=pass_buf.at[m, tile_at(h, piece)],
            dst_ref=grad_buf.at[m, tile_at(h, piece)],
            send_sem=down_send.at[m, h],
            recv_sem=down_recv.at[m, h],
            device_id={"section": target},
            device_id_type=pl.DeviceIdType.MESH,
        )

    def gain_copy(owner, bits):
        return pltpu.make_async_remote_copy(
            src_ref=gain_all.at[owner],
            dst_ref=gain_all.at[owner],
            send_sem=gain_send.at[bits],
            recv_sem=gain_recv.at[bits],
            device_id=peer(bits),
            device_id_type=pl.DeviceIdType.MESH,
        )

    barrier = pltpu.get_barrier_semaphore()
    for bits in range(1, peers):
        pl.semaphore_signal(
            barrier, inc=1, device_id=peer(bits), device_id_type=pl.DeviceIdType.MESH
        )

    @pl.when(section > 0)
    def _():
        pl.semaphore_signal(
            barrier,
            inc=1,
            device_id={"section": section - 1},
            device_id_type=pl.DeviceIdType.MESH,
        )

    @pl.when(section < sections - 1)
    def _():
        pl.semaphore_signal(
            barrier,
            inc=1,
            device_id={"section": section + 1},
            device_id_type=pl.DeviceIdType.MESH,
        )

    pl.semaphore_wait(
        barrier,
        peers - 1
        + (section > 0).astype(jnp.int32)
        + (section < sections - 1).astype(jnp.int32),
    )

    gain_all[me] = jnp.zeros((1, width), jnp.float32)
    vg_ref[...] = jnp.zeros_like(vg_ref)
    og_ref[...] = jnp.zeros_like(og_ref)

    def scales(m, carry):
        slot = slot_ref[0, m]

        def squares(j, total):
            x = saved_ref[slot, :, tile_at(j)].astype(jnp.float32)
            return total + jnp.sum(x * x, axis=1, keepdims=True)

        total = lax.fori_loop(0, wide, squares, jnp.zeros((tokens, 1), jnp.float32))
        inv_buf[m] = lax.rsqrt(total / width + EPSILON)
        return carry

    lax.fori_loop(0, micro, scales, 0)
    for load in loads:
        load.wait()

    def send_cols(kind, m):
        cols_all[kind, m, :, tile_at(me, tokens)] = turned[kind, m, tile_at(me, share)]
        for bits in range(1, peers):
            col_copy(kind, m, me, bits).start()

    def send_rows(kind, m):
        for bits in (*range(2, peers, 2), 1):
            own_rows(kind, m, bits).start()

    def values(m):
        slot = slot_ref[0, m]
        inv = inv_buf[m]

        def norm(j, carry):
            x = saved_ref[slot, :, tile_at(j)].astype(jnp.float32)
            n = (x * inv * gain_ref[:, tile_at(j)]).astype(jnp.bfloat16)
            pass_tile[:, tile_at(j)] = n
            turned[0, m, tile_at(j)] = n.T
            return carry

        lax.fori_loop(0, wide, norm, 0)
        send_cols(0, m)

        def project(j, carry):
            rows_all[0, m, tile_at(me, tokens), tile_at(j)] = jnp.dot(
                pass_tile[...], wv_ref[:, tile_at(j)], preferred_element_type=jnp.float32
            ).astype(jnp.bfloat16)
            return carry

        lax.fori_loop(0, narrow, project, 0)
        send_rows(0, m)

    pass_tile = gn_buf[0]
    gn = gn_buf[1]

    def chain(m):
        slot = slot_ref[0, m]

        @pl.when(top)
        def _():
            grad_buf[m] = cot_ref[m]

        def one_piece(h, done):
            rows = tile_at(h, piece)
            own = tile_at(me * PIECES + h, piece)
            inv = inv_buf[m, rows]

            @pl.when(section < sections - 1)
            def _():
                down_copy(m, h, section + 1).wait_recv()

            def project(j, carry):
                rows_all[1, m, own, tile_at(j)] = jnp.dot(
                    grad_buf[m, rows], wo_ref[:, tile_at(j)], preferred_element_type=jnp.float32
                ).astype(jnp.bfloat16)
                return carry

            lax.fori_loop(0, narrow, project, 0)

            def back(j, total):
                term = lax.dot_general(
                    rows_all[1, m, own],
                    wv_ref[tile_at(j)],
                    (((1,), (1,)), ((), ())),
                    preferred_element_type=jnp.float32,
                )
                unit = saved_ref[slot, rows, tile_at(j)].astype(jnp.float32) * inv
                gn[rows, tile_at(j)] = term
                both = term * unit
                gain_all[me, :, tile_at(j)] += jnp.sum(both, axis=0, keepdims=True)
                return total + jnp.sum(both * gain_ref[:, tile_at(j)], axis=1, keepdims=True)

            total = lax.fori_loop(0, wide, back, jnp.zeros((piece, 1), jnp.float32))
            mean = total / width

            @pl.when(section > 0)
            def _():
                def step(j, carry):
                    unit = saved_ref[slot, rows, tile_at(j)].astype(jnp.float32) * inv
                    grad_unit = gn[rows, tile_at(j)] * gain_ref[:, tile_at(j)]
                    pass_buf[m, rows, tile_at(j)] = (
                        grad_buf[m, rows, tile_at(j)].astype(jnp.float32)
                        + inv * (grad_unit - unit * mean)
                    ).astype(jnp.bfloat16)
                    return carry

                lax.fori_loop(0, wide, step, 0)
                down_copy(m, h, section - 1).start()

            return done

        lax.fori_loop(0, PIECES, one_piece, 0)
        send_rows(1, m)

        def turn(j, carry):
            turned[1, m, tile_at(j)] = grad_buf[m, :, tile_at(j)].T
            return carry

        lax.fori_loop(0, wide, turn, 0)
        send_cols(1, m)

    def stage(t, carry):
        at_top = top.astype(jnp.int32)
        chained = at_top * (1 - t % 2) + (1 - at_top) * (t // micro)
        m = at_top * (t // 2) + (1 - at_top) * (t % micro)

        @pl.when(chained == 1)
        def _():
            chain(m)

        @pl.when(chained == 0)
        def _():
            values(m)

        return carry

    lax.fori_loop(0, 2 * micro, stage, 0)
    for bits in range(1, peers):
        gain_copy(me, bits).start()

    def finish(m, carry):
        for kind in (0, 1):
            for bits in range(2, peers, 2):
                arriving_rows(kind, m, bits).wait_recv()
                relayed_rows(kind, m, bits).start()
        for kind in (0, 1):
            for bits in range(1, peers):
                col_copy(kind, m, flipped(me, bits, peers), bits).wait_recv()
        for kind in (0, 1):
            for bits in range(1, peers, 2):
                arriving_rows(kind, m, bits).wait_recv()

        def weight(j, inside):
            vg_ref[:, tile_at(j)] += jnp.dot(
                cols_all[0, m], rows_all[1, m, :, tile_at(j)], preferred_element_type=jnp.float32
            )
            og_ref[:, tile_at(j)] += jnp.dot(
                cols_all[1, m], rows_all[0, m, :, tile_at(j)], preferred_element_type=jnp.float32
            )
            return inside

        lax.fori_loop(0, narrow, weight, 0)
        return carry

    lax.fori_loop(0, micro, finish, 0)
    for bits in range(1, peers):
        gain_copy(flipped(me, bits, peers), bits).wait_recv()
    gained = gain_all[0]
    for owner in range(1, peers):
        gained = gained + gain_all[owner]
    gg_ref[...] = gained

    def drain(m, carry):
        for kind in (0, 1):
            for bits in range(1, peers):
                col_copy(kind, m, me, bits).wait_send()
            for bits in (1, *range(2, peers, 2)):
                own_rows(kind, m, bits).wait_send()
            for bits in range(2, peers, 2):
                relayed_rows(kind, m, bits).wait_send()

        @pl.when(section > 0)
        def _():
            for h in range(PIECES):
                down_copy(m, h, section - 1).wait_send()

        return carry

    lax.fori_loop(0, micro, drain, 0)
    for bits in range(1, peers):
        gain_copy(me, bits).wait_send()


def fused(mesh, saved, cotangent, slot_table, gain, value_weight, out_weight):
    peers, sections = mesh.shape["seq"], mesh.shape["section"]
    micro, tokens, width = cotangent.shape
    inner = value_weight.shape[2]
    share = width // peers
    whole = pl.BlockSpec(memory_space=pltpu.VMEM)
    value_grad, out_grad, gain_grad = pl.pallas_call(
        functools.partial(fused_kernel, peers, sections),
        out_shape=(
            jax.ShapeDtypeStruct((share, inner), jnp.float32),
            jax.ShapeDtypeStruct((share, inner), jnp.float32),
            jax.ShapeDtypeStruct((1, width), jnp.float32),
        ),
        in_specs=[pl.BlockSpec(memory_space=pltpu.SMEM)] + [whole] * 3
        + [pl.BlockSpec(memory_space=pl.ANY)] * 2,
        out_specs=(whole, whole, whole),
        scratch_shapes=[
            pltpu.VMEM((micro, tokens, 1), jnp.float32),
            pltpu.VMEM((micro, tokens, width), jnp.bfloat16),
            pltpu.VMEM((micro, tokens, width), jnp.bfloat16),
            (pltpu.VMEM((tokens, width), jnp.bfloat16), pltpu.VMEM((tokens, width), jnp.float32)),
            pltpu.VMEM((2, micro, peers * tokens, inner), jnp.bfloat16),
            pltpu.VMEM((2, micro, width, tokens), jnp.bfloat16),
            pltpu.VMEM((2, micro, share, peers * tokens), jnp.bfloat16),
            pltpu.VMEM((peers, 1, width), jnp.float32),
            pltpu.SemaphoreType.DMA((2, micro, peers)),
            pltpu.SemaphoreType.DMA((2, micro, peers)),
            pltpu.SemaphoreType.DMA((2, micro, peers)),
            pltpu.SemaphoreType.DMA((2, micro, peers)),
            pltpu.SemaphoreType.DMA((micro, PIECES)),
            pltpu.SemaphoreType.DMA((micro, PIECES)),
            pltpu.SemaphoreType.DMA((peers,)),
            pltpu.SemaphoreType.DMA((peers,)),
            pltpu.VMEM((width, inner), jnp.bfloat16),
            pltpu.VMEM((width, inner), jnp.bfloat16),
            pltpu.SemaphoreType.DMA((2,)),
        ],
        compiler_params=pltpu.CompilerParams(
            collective_id=0, has_side_effects=True, vmem_limit_bytes=VMEM_BYTES
        ),
    )(slot_table, saved[0], cotangent, gain, value_weight[0], out_weight[0])
    return value_grad[None], out_grad[None], gain_grad


def fits(mesh, saved, cotangent, slot_table, gain, value_weight, out_weight):
    peers = mesh.shape["seq"]
    micro, tokens, width = cotangent.shape
    inner = value_weight.shape[2]
    held = 4 * width * inner + 4 * micro * tokens * (2 * width + inner * peers)
    held += 4 * micro * tokens * width * 3 + 8 * (width // peers) * inner + 6 * tokens * width
    return (
        peers & (peers - 1) == 0
        and tokens % LANES == 0
        and width % TILE == 0
        and inner % TILE == 0
        and width % (16 * peers) == 0
        and held < VMEM_BYTES - 4 * 1024 * 1024
    )


def on_device(mesh, *arrays):
    if fits(mesh, *arrays):
        return fused(mesh, *arrays)
    return per_device(*arrays)


def solution(mesh):
    in_specs = (
        P("section", None, "seq", None),
        P(None, "seq", None),
        P("section", None),
        P("section", None),
        P("section", None, None),
        P("section", None, None),
    )
    out_specs = (P("section", "seq", None), P("section", "seq", None), P("section", None))
    return jax.shard_map(
        functools.partial(on_device, mesh), mesh=mesh, in_specs=in_specs, out_specs=out_specs, check_vma=False
    )
```
